32 devices in a mesh: row: 4 (over x, core), seq: 8 (over z, y).
Axes of the slice: x: 2, y: 2, z: 4, core: 2. Of those that a mesh axis runs over, the one named last changes fastest.
Arguments:
- tokens_in: bfloat16 [4, 2048, 1024], P('row', 'seq'), may hold values from -6 to 6
- segment_ids: int32 [4, 2048], P('row'), may hold values from 0 to 15, never falling along the last dimension, each value on 1 to 1024 neighbouring positions
- norm_in_gain: float32 [1024], replicated, may hold values from 0.5 to 1.5
- query_weight: bfloat16 [1024, 1024], replicated, may hold values from -0.1875 to 0.1875
- key_weight: bfloat16 [1024, 1024], replicated, may hold values from -0.1875 to 0.1875
- value_weight: bfloat16 [1024, 1024], replicated, may hold values from -0.1875 to 0.1875
- rate_weight: bfloat16 [1024, 16], replicated, may hold values from -0.1875 to 0.1875
- gate_weight: bfloat16 [1024, 1024], replicated, may hold values from -0.1875 to 0.1875
- out_weight: bfloat16 [1024, 1024], replicated, may hold values from -0.1875 to 0.1875
- state_init: float32 [16, 64, 64], P('seq'), may hold values from -0.75 to 0.75
- offset_init: float32 [16, 64], P('seq'), may hold values from -3 to 3
- inner_gain: float32 [16, 64], P('seq'), may hold values from 0.5 to 1.5
- inner_shift: float32 [16, 64], P('seq'), may hold values from -3 to 3
- rate_bias: float32 [16], P('seq'), may hold values from -2 to 2
- norm_post_gain: float32 [1024], replicated, may hold values from 0.5 to 1.5
- norm_mlp_gain: float32 [1024], replicated, may hold values from 0.5 to 1.5
- ffn_gate: bfloat16 [1024, 2736], replicated, may hold values from -0.1875 to 0.1875
- ffn_up: bfloat16 [1024, 2736], replicated, may hold values from -0.1875 to 0.1875
- ffn_down: bfloat16 [2736, 1024], replicated, may hold values from -0.109375 to 0.109375
- cotangent: bfloat16 [4, 2048, 1024], P('row', 'seq'), may hold values from -6 to 6
Outputs:
- block_out: bfloat16 [4, 2048, 1024], P('row', 'seq')
- grad_tokens: float32 [4, 2048, 1024], P('row', 'seq')
- grad_norm_in: float32 [1024], P(('row', 'seq'))
- grad_query: float32 [1024, 1024], P(('row', 'seq'))
- grad_key: float32 [1024, 1024], P(('row', 'seq'))
- grad_value: float32 [1024, 1024], P(('row', 'seq'))
- grad_rate: float32 [1024, 16], P(('row', 'seq'))
- grad_gate: float32 [1024, 1024], P(('row', 'seq'))
- grad_out_proj: float32 [1024, 1024], P(('row', 'seq'))
- grad_state_init: float32 [16, 64, 64], P('seq')
- grad_offset_init: float32 [16, 64], P('seq')
- grad_inner_gain: float32 [16, 64], P('seq')
- grad_inner_shift: float32 [16, 64], P('seq')
- grad_rate_bias: float32 [16], P('seq')
- grad_norm_post: float32 [1024], P(('row', 'seq'))
- grad_norm_mlp: float32 [1024], P(('row', 'seq'))
- grad_ffn_gate: float32 [1024, 2736], P(('row', 'seq'))
- grad_ffn_up: float32 [1024, 2736], P(('row', 'seq'))
- grad_ffn_down: float32 [2736, 1024], P(None, ('row', 'seq'))
The draws below stay inside these ranges and needn't reach their ends.
Inputs may be any that keep to these rules, and one draw needn't show every extreme that they name: Along a row segment_ids never fall; a document is a run of equal ids of at most 1024 tokens.
All inputs are finite; a program needn't handle non-finite values.
Results may differ from the reference program's by a relative error of at most 0.018.
Values may be sent and summed in bfloat16 or wider, within the bound.
A program may use at most 256 MiB of HBM per device.

```python
import math
import jax
import jax.numpy as jnp
import numpy as np
from jax import lax

D = 1024
H = 16
HS = 64
FF = 2736
MB = 16
MB_BLOCK = 8
LEN = 2048
ROWS = 4


def steps_of(key, dims, cuts, smallest, high):
    factor_of = 1.0
    for axis_at, parts in cuts:
        steps = jax.random.uniform(jax.random.fold_in(jax.random.fold_in(key, 6), axis_at), (parts,), jnp.float32, smallest / len(cuts), high / len(cuts))
        factor_of = factor_of * jnp.repeat(jnp.exp(steps), dims[axis_at] // parts).reshape((-1,) + (1,) * (len(dims) - 1 - axis_at))
    return factor_of


def length_profile(count, total, bound, skew):
    loads = [(1 << 20) // math.isqrt(rank ** skew) + 1 for rank in range(2, count + 1)]
    spare, counts = total - bound - (count - 1), [1] * (count - 1)
    while spare > 0:
        free = [i for i in range(count - 1) if counts[i] < bound]
        mass, budget = sum([loads[i] for i in free]), spare
        for i in free:
            extra = min(bound - counts[i], max(1, budget * loads[i] // mass), spare)
            counts[i] = counts[i] + extra
            spare = spare - extra
    return np.array([bound] + counts)


def ragged(stream_key, amount, total, bound, slope):
    if amount == 2:
        one = jax.random.randint(stream_key, (), max(1, total - bound), min(bound, total - 1) + 1)
        return jnp.stack([one, total - one])
    sizes = jnp.asarray(length_profile(amount, total, bound, slope), jnp.int32)
    couples = (amount - 1) // 2
    donor, receiver = sizes[1:1 + 2 * couples:2], sizes[2:2 + 2 * couples:2]
    margin = jnp.minimum(donor - 1, bound - receiver)
    moved = jax.random.randint(jax.random.fold_in(stream_key, 1), (couples,), 0, 1 << 20) % (margin + 1)
    sizes = sizes.at[1:1 + 2 * couples:2].set(donor - moved).at[2:2 + 2 * couples:2].set(receiver + moved)
    return sizes[jax.random.permutation(jax.random.fold_in(stream_key, 2), amount)]


def normal_values(key, dims, deviation, most, split=(), held_as=jnp.bfloat16):
    drawn = jax.random.normal(key, dims, jnp.float32) * deviation
    if len(split) > 0:
        drawn = steps_of(key, dims, split, -0.22, 0.18) * drawn
    return jnp.clip(drawn, min=-most, max=most).astype(held_as)


def setup_inputs(seed: int = 0) -> dict:
    arg_keys = jax.random.split(jax.random.key(seed), 21)
    return {
        "tokens_in": normal_values(arg_keys[0], (ROWS, LEN, D), 1.0, 6.0, ((0, 4), (1, 8))),
        "segment_ids": jax.vmap(lambda own: jnp.searchsorted(jnp.cumsum(ragged(own, LEN // 128, LEN, LEN // 2, 2)), jnp.arange(LEN), side="right"))(jax.random.split(arg_keys[1], ROWS)).reshape((ROWS, LEN)).astype(jnp.int32),
        "norm_in_gain": jnp.clip(1.0 + 0.1 * jax.random.normal(arg_keys[2], (D,), jnp.float32), 0.5, 1.5),
        "query_weight": normal_values(arg_keys[3], (D, D), D ** -0.5, 0.1875),
        "key_weight": normal_values(arg_keys[4], (D, D), D ** -0.5, 0.1875),
        "value_weight": normal_values(arg_keys[5], (D, D), D ** -0.5, 0.1875),
        "rate_weight": normal_values(arg_keys[6], (D, H), D ** -0.5, 0.1875),
        "gate_weight": normal_values(arg_keys[7], (D, D), D ** -0.5, 0.1875),
        "out_weight": normal_values(arg_keys[8], (D, D), D ** -0.5, 0.1875),
        "state_init": normal_values(arg_keys[9], (H, HS, HS), HS ** -0.5, 0.75, ((0, 8),), jnp.float32),
        "offset_init": normal_values(arg_keys[10], (H, HS), 0.5, 3.0, ((0, 8),), jnp.float32),
        "inner_gain": jnp.clip(1.0 + 0.1 * jax.random.normal(arg_keys[11], (H, HS), jnp.float32), 0.5, 1.5),
        "inner_shift": normal_values(arg_keys[12], (H, HS), 0.5, 3.0, ((0, 8),), jnp.float32),
        "rate_bias": jnp.clip(jax.random.uniform(arg_keys[13], (H,), jnp.float32, -2.0, 2.0) * steps_of(arg_keys[13], (H,), ((0, 8),), -0.4, 0.0), -2.0, 2.0),
        "norm_post_gain": jnp.clip(1.0 + 0.1 * jax.random.normal(arg_keys[14], (D,), jnp.float32), 0.5, 1.5),
        "norm_mlp_gain": jnp.clip(1.0 + 0.1 * jax.random.normal(arg_keys[15], (D,), jnp.float32), 0.5, 1.5),
        "ffn_gate": normal_values(arg_keys[16], (D, FF), D ** -0.5, 0.1875),
        "ffn_up": normal_values(arg_keys[17], (D, FF), D ** -0.5, 0.1875),
        "ffn_down": normal_values(arg_keys[18], (FF, D), FF ** -0.5, 0.109375),
        "cotangent": normal_values(arg_keys[19], (ROWS, LEN, D), 1.0, 6.0, ((0, 4), (1, 8))),
    }


EPS = 1e-06
BASE_LR = 1.0
HIGHEST = lax.Precision.HIGHEST

@jax.custom_vjp
def low(v):
    return lax.optimization_barrier(v.astype(jnp.bfloat16)).astype(jnp.float32)

@jax.custom_vjp
def low_back(v):
    return v

def low_keep(v):
    return (low(v), None)

def low_pass(kept, grad):
    return (grad,)

def back_keep(v):
    return (v, None)

def back_low(kept, grad):
    return (low(grad),)
low.defvjp(low_keep, low_pass)
low_back.defvjp(back_keep, back_low)

def matmul(left, right):
    return jnp.dot(left, right, precision=HIGHEST)

def rms_scale(values, gain):
    return values * lax.rsqrt(lax.optimization_barrier(jnp.mean(values * values, axis=-1, keepdims=True)) + EPS) * gain

def layer_norm(values):
    center = values - lax.optimization_barrier(jnp.mean(values, axis=-1, keepdims=True))
    inverse = lax.rsqrt(lax.optimization_barrier(jnp.mean(center * center, axis=-1, keepdims=True)) + EPS)
    return (center * inverse, inverse)

def mini_batch(carried, queries, keys_in, values_in, step_rate, segment, state_zero, offset_zero, norm_gain, norm_shift):
    weight, offset, last_seg = carried
    length = queries.shape[1]
    continues = (segment == last_seg[:, None]).astype(jnp.float32)[:, :, None]

    def starting(inputs):
        from_state = jnp.einsum('bih,bhe->bie', inputs, weight, precision=HIGHEST) + offset[:, None, :]
        from_zero = jnp.einsum('bih,bhe->bie', inputs, state_zero, precision=HIGHEST) + offset_zero[:, None, :]
        return continues * from_state + (1.0 - continues) * from_zero
    gain_row = norm_gain[:, None, :]
    shift_row = norm_shift[:, None, :]
    normed, inverse = layer_norm(starting(keys_in))
    residue = gain_row * normed + shift_row - (values_in - keys_in)
    scaled = residue * gain_row
    grad_inner = inverse * (scaled - lax.optimization_barrier(jnp.mean(scaled, axis=-1, keepdims=True)) - normed * lax.optimization_barrier(jnp.mean(scaled * normed, axis=-1, keepdims=True)))
    positions = jnp.arange(length)
    causal = positions[None, :] <= positions[:, None]
    same_doc = (segment[:, :, None] == segment[:, None, :]) & causal[None, :, :]
    divisor = jnp.arange(1, length + 1).astype(jnp.float32)
    step_sizes = step_rate[:, None, :] / divisor[None, :, None] * same_doc.astype(jnp.float32)
    scores = jnp.einsum('bih,bjh->bij', queries, keys_in, precision=HIGHEST) + 1.0
    inner_out = starting(queries) - jnp.einsum('bij,bjh->bih', step_sizes * scores, grad_inner, precision=HIGHEST)
    final_norm, unused = layer_norm(inner_out)
    results = queries + gain_row * final_norm + shift_row
    last_cont = continues[:, -1, :]
    last_steps = step_sizes[:, -1, :]
    base_weight = last_cont[:, :, None] * weight + (1.0 - last_cont[:, :, None]) * state_zero
    base_offset = last_cont * offset + (1.0 - last_cont) * offset_zero
    new_weight = base_weight - jnp.einsum('bj,bjh,bje->bhe', last_steps, keys_in, grad_inner, precision=HIGHEST)
    new_offset = base_offset - jnp.einsum('bj,bje->be', last_steps, grad_inner, precision=HIGHEST)
    return ((new_weight, new_offset, segment[:, -1]), results)

def inner_loop(queries, keys_in, values_in, logits, segments, state_zero, offset_zero, norm_gain, norm_shift, rate_bias, checkpointed):
    batches, length, features = queries.shape
    block_len = MB * MB_BLOCK
    num_blocks = length // block_len
    step_rate = BASE_LR * jax.nn.sigmoid(logits + rate_bias[:, None]) / features

    def blocked(values):
        shaped = values.reshape((batches, num_blocks, block_len) + values.shape[2:])
        return jnp.swapaxes(shaped, 0, 1)

    def block_step(carried, inputs):
        query_blk, key_blk, value_blk, rate_blk, segment_blk = inputs
        pieces = []
        for number in range(MB_BLOCK):
            first_pos = number * MB
            last_pos = first_pos + MB
            carried, result = mini_batch(carried, query_blk[:, first_pos:last_pos], key_blk[:, first_pos:last_pos], value_blk[:, first_pos:last_pos], rate_blk[:, first_pos:last_pos], segment_blk[:, first_pos:last_pos], state_zero, offset_zero, norm_gain, norm_shift)
            pieces.append(result)
        return (carried, jnp.concatenate(pieces, axis=1))
    stepper = jax.checkpoint(block_step) if checkpointed else block_step
    initial = (state_zero, offset_zero, jnp.full((batches,), -1, jnp.int32))
    unused, results = lax.scan(stepper, initial, (blocked(queries), blocked(keys_in), blocked(values_in), blocked(step_rate), blocked(segments)))
    return jnp.swapaxes(results, 0, 1).reshape(batches, length, features)

def one_row(params, tokens_row, segment_row):
    norm_in_gain, query_weight, key_weight, value_weight, rate_weight, gate_weight, out_weight, state_init, offset_init, inner_gain, inner_shift, rate_bias, norm_post_gain, norm_mlp_gain, ffn_gate, ffn_up, ffn_down = params
    length = tokens_row.shape[0]
    normed_in = low(rms_scale(tokens_row, norm_in_gain))

    def project(weight):
        return low(low_back(matmul(normed_in, weight)))

    def split_heads(values):
        return jnp.transpose(values.reshape(length, H, HS), (1, 0, 2))
    queries = project(query_weight)
    keys_all = project(key_weight)
    values_all = project(value_weight)
    rate_logits = project(rate_weight)
    seg_heads = jnp.broadcast_to(segment_row[None, :], (H, length))
    mixed_heads = inner_loop(split_heads(queries), split_heads(keys_all), split_heads(values_all), jnp.transpose(rate_logits), seg_heads, state_init, offset_init, inner_gain, inner_shift, rate_bias, True)
    mixed = low(low_back(jnp.transpose(mixed_heads, (1, 0, 2)).reshape(length, D)))
    post_norm = rms_scale(mixed, norm_post_gain)
    gate_pre = low_back(matmul(normed_in, gate_weight))
    branch = low(post_norm * jax.nn.gelu(gate_pre, approximate=True))
    middle = tokens_row + low_back(matmul(branch, out_weight))
    normed_mid = low(rms_scale(middle, norm_mlp_gain))
    gate_proj = low_back(matmul(normed_mid, ffn_gate))
    up_proj = low_back(matmul(normed_mid, ffn_up))
    hidden = low(jax.nn.silu(gate_proj) * up_proj)
    return middle + low_back(matmul(hidden, ffn_down))

def reference(tokens_in, segment_ids, norm_in_gain, query_weight, key_weight, value_weight, rate_weight, gate_weight, out_weight, state_init, offset_init, inner_gain, inner_shift, rate_bias, norm_post_gain, norm_mlp_gain, ffn_gate, ffn_up, ffn_down, cotangent):
    raw = (norm_in_gain, query_weight, key_weight, value_weight, rate_weight, gate_weight, out_weight, state_init, offset_init, inner_gain, inner_shift, rate_bias, norm_post_gain, norm_mlp_gain, ffn_gate, ffn_up, ffn_down)
    params = tuple((member.astype(jnp.float32) for member in raw))

    def add_up(first, second):
        return first + second

    def row_step(totals, row_inputs):
        tokens_row, segment_row, cot_row = row_inputs

        def forward(weights_all, tokens_here):
            return one_row(weights_all, tokens_here, segment_row)
        output, pullback = jax.vjp(forward, params, tokens_row)
        grad_params, grad_row = pullback(cot_row)
        totals = jax.tree.map(add_up, totals, grad_params)
        return (totals, (output.astype(jnp.bfloat16), grad_row))
    zeros_init = jax.tree.map(jnp.zeros_like, params)
    totals, outputs = lax.scan(row_step, zeros_init, (tokens_in.astype(jnp.float32), segment_ids, cotangent.astype(jnp.float32)))
    block_out, grad_tokens = outputs
    return (block_out, grad_tokens, totals[0], totals[1], totals[2], totals[3], totals[4], totals[5], totals[6], totals[7], totals[8], totals[9], totals[10], totals[11], totals[12], totals[13], totals[14], totals[15], totals[16])
```

```python
import functools
import jax
import jax.numpy as jnp
import numpy as np
from jax import lax
from jax.experimental import pallas as pl
from jax.experimental.pallas import tpu as pltpu
from jax.sharding import PartitionSpec as P

MB = 16
BLK = 128
EPS = 1e-06
F32 = jnp.float32
BF = jnp.bfloat16


def dot(a, b):
    return lax.dot_general(a, b, (((1,), (0,)), ((), ())), preferred_element_type=F32)


def dot_nt(a, b):
    return lax.dot_general(a, b, (((1,), (1,)), ((), ())), preferred_element_type=F32)


def dot_tn(a, b):
    return lax.dot_general(a, b, (((0,), (0,)), ((), ())), preferred_element_type=F32)


def split(x):
    hi = x.astype(BF)
    return hi, (x - hi.astype(F32)).astype(BF)


def head_blocks(lanes, size):
    shape = (lanes, lanes)
    return lax.broadcasted_iota(jnp.int32, shape, 0) // size == lax.broadcasted_iota(jnp.int32, shape, 1) // size


def mean_matrix(lanes, size):
    return jnp.where(head_blocks(lanes, size), 1.0 / size, 0.0).astype(BF)


def head_mean(x, means):
    hi, lo = split(x)
    return dot(hi, means) + dot(lo, means)


def lane_mean(x, size):
    lanes = x.shape[-1]
    if lanes == size:
        return jnp.sum(x, axis=-1, keepdims=True) * (1.0 / size)
    at = lax.broadcasted_iota(jnp.int32, x.shape, 1) // size
    out = None
    for h in range(lanes // size):
        part = jnp.sum(jnp.where(at == h, x, 0.0), axis=-1, keepdims=True) * (1.0 / size)
        out = part if out is None else jnp.where(at == h, part, out)
    return out


def lane_schedule(segments):
    count = segments.shape[0] // MB
    last = segments[MB - 1::MB]
    before = jnp.concatenate([jnp.full((1,), -1, jnp.int32), last[:-1]])
    fresh = last != before
    at = jnp.arange(count, dtype=jnp.int32)
    first, stop = at[:, None], at[None, :] + 1
    stop_ok = jnp.concatenate([fresh[1:], jnp.ones((1,), bool)])
    steps0 = first + 1 + count - stop
    steps1 = jnp.where(stop < count, stop - first + 1, count - first)
    cost = jnp.where(fresh[:, None] & stop_ok[None, :] & (stop > first), jnp.maximum(steps0, steps1), 4 * count)
    best = jnp.argmin(cost.reshape(-1)).astype(jnp.int32)
    a, b = best // count, best % count + 1
    end = jnp.minimum(b, count - 1)
    steps = jnp.maximum(a + 1 + count - b, end - a + 1)
    t = jnp.arange(count + 2, dtype=jnp.int32)
    per = BLK // MB

    def table(where, valid, owned, edge):
        where_ok = jnp.where(valid, where, count - 1)
        write = jnp.where(valid & owned, where, count)
        slot = jnp.where(valid & owned & (where % per == edge), where // per, count // per)
        return jnp.stack([where_ok, write, slot])

    f0 = jnp.where(t <= a, t, t - a - 1 + b)
    f1 = a + t
    fwd = jnp.stack([table(f0, f0 < count, (t <= a) | (f0 > b), 0), table(f1, f1 <= end, f1 > a, 0)])
    r0 = jnp.where(t < count - b, count - 1 - t, a - (t - (count - b)))
    r1 = end - t
    bwd = jnp.stack([table(r0, r0 >= 0, (r0 >= b) | (r0 < a), per - 1), table(r1, r1 >= a, r1 < b, per - 1)])
    return steps.reshape(1), fwd, bwd, jnp.concatenate([jnp.full((1,), -1, jnp.int32), last])


def scan_fwd_kernel(size, mean_of, steps_ref, table_ref, last_ref, k_ref, v_ref, seg_ref, rate_ref, wz_ref, bz_ref, gain_ref, shift_ref,
                    z_ref, g_ref, s_ref, b_ref, z0_ref, pd_ref, m5_ref, zb_ref, gb_ref, sw_ref, s2_ref, bw_ref):
    tokens, lanes = k_ref.shape
    count = tokens // MB
    mask = head_blocks(lanes, size)
    means = mean_matrix(lanes, size)
    gain, shift = gain_ref[...], shift_ref[...]
    gain2 = gain * gain
    wz_hi, wz_lo = split(wz_ref[...])
    bz = bz_ref[...]

    @pl.loop(0, tokens // 256)
    def _(n):
        rows = pl.ds(pl.multiple_of(n * 256, 256), 256)
        k = k_ref[rows, :]
        z0_ref[rows, :] = dot(k, wz_hi) + dot(k, wz_lo) + bz
        pd = gain * (shift - (v_ref[rows, :].astype(F32) - k.astype(F32)))
        pd_ref[rows, :] = pd
        m5_ref[rows, :] = head_mean(pd, means)

    sw_ref[...] = jnp.zeros_like(sw_ref)
    s2_ref[...] = jnp.zeros_like(s2_ref)
    bw_ref[...] = jnp.zeros_like(bw_ref)

    def step(t, carry):
        for lane in range(2):
            m, write, slot = table_ref[lane, 0, t], table_ref[lane, 1, t], table_ref[lane, 2, t]
            rows = pl.ds(pl.multiple_of(m * MB, MB), MB)
            to = pl.ds(pl.multiple_of(write * MB, MB), MB)
            last_before, last_here = last_ref[m], last_ref[m + 1]
            k = k_ref[rows, :]
            seg = seg_ref[rows, :]
            bias = bw_ref[lane, 0:1, :]
            state = sw_ref[lane]
            s_ref[slot] = state
            b_ref[slot] = bw_ref[lane]
            zc = dot(jnp.concatenate([k, k], axis=1), s2_ref[lane]) + bias
            z = z0_ref[rows, :] + jnp.where(seg == last_before, zc, 0.0)
            pd = pd_ref[rows, :]
            gz = gain2 * z
            q1, q2, q3, q4 = mean_of(z * z), mean_of(gz), mean_of(gz * z), mean_of(pd * z)
            s = lax.rsqrt(q1 + EPS)
            m1 = s * q2 + m5_ref[rows, :]
            m2 = s * (s * q3 + q4)
            g = s * ((gain2 - m2) * (s * z) + (pd - m1))
            rho = jnp.where(seg == last_here, rate_ref[rows, :], 0.0) * (1.0 / MB)
            step_g = rho * g
            zb_ref[to, :] = z
            gb_ref[to, :] = g
            hi, lo = split(step_g)
            delta = dot_tn(jnp.concatenate([k, k], axis=0), jnp.concatenate([hi, lo], axis=0))
            keep = jnp.where(last_before == last_here, 1.0, 0.0)
            state = keep * state - jnp.where(mask, delta, 0.0)
            sw_ref[lane] = state
            s_hi, s_lo = split(state)
            s2_ref[lane] = jnp.concatenate([s_hi, s_lo], axis=0)
            bw_ref[lane] = keep * bw_ref[lane] - jnp.sum(step_g, axis=0, keepdims=True)
        return carry

    lax.fori_loop(0, steps_ref[0], step, 0)
    z_ref[...] = zb_ref[0:tokens, :]
    g_ref[...] = gb_ref[0:tokens, :]


def smem():
    return pl.BlockSpec(memory_space=pltpu.SMEM)


def vmem():
    return pl.BlockSpec(memory_space=pltpu.VMEM)


def scan_fwd(schedule, k, v, seg, rate, wz, bz, gain, shift, size, mean_of):
    steps, table, _, last = schedule
    tokens, lanes = k.shape
    blocks = tokens // BLK
    return pl.pallas_call(
        functools.partial(scan_fwd_kernel, size, mean_of),
        out_shape=(
            jax.ShapeDtypeStruct((tokens, lanes), F32),
            jax.ShapeDtypeStruct((tokens, lanes), F32),
            jax.ShapeDtypeStruct((blocks + 1, lanes, lanes), F32),
            jax.ShapeDtypeStruct((blocks + 1, 8, lanes), F32),
        ),
        in_specs=[smem()] * 3 + [vmem()] * 8,
        out_specs=(vmem(),) * 4,
        scratch_shapes=[
            pltpu.VMEM((tokens, lanes), F32),
            pltpu.VMEM((tokens, lanes), F32),
            pltpu.VMEM((tokens, lanes), F32),
            pltpu.VMEM((tokens + MB, lanes), F32),
            pltpu.VMEM((tokens + MB, lanes), F32),
            pltpu.VMEM((2, lanes, lanes), F32),
            pltpu.VMEM((2, 2 * lanes, lanes), BF),
            pltpu.VMEM((2, 8, lanes), F32),
        ],
        compiler_params=pltpu.CompilerParams(vmem_limit_bytes=60 * 1024 * 1024),
        name="scan_fwd",
    )(steps, table, last, k, v, seg, rate, wz, bz, gain, shift)


def weights_of(segments):
    blocks = segments.shape[0] // BLK
    seg = segments.reshape(blocks, BLK)
    same = seg[:, :, None] == seg[:, None, :]
    at = jnp.arange(BLK)
    mb = at // MB
    inside = (mb[:, None] == mb[None, :]) & (at[None, :] <= at[:, None])
    part = inside / (at % MB + 1).astype(F32)[:, None] + (mb[None, :] < mb[:, None]) * (1.0 / MB)
    return (same * part[None]).astype(F32).reshape(blocks * BLK, BLK)


def head_masks(shape, size):
    at = lax.broadcasted_iota(jnp.int32, shape, 1) // size
    return [at == h for h in range(shape[1] // size)]


def only(mask, x):
    return jnp.where(mask, x, jnp.zeros_like(x))


def layer_norm_parts(o, means):
    center = o - head_mean(o, means)
    inverse = lax.rsqrt(head_mean(center * center, means) + EPS)
    return center * inverse, inverse


def out_fwd_kernel(size, seg_before_ref, q_ref, k_ref, g_ref, rate_ref, seg_ref, w_ref, s_ref, b_ref, wz_ref, bz_ref, gain_ref, shift_ref,
                   mixed_ref, fin_ref, inv_ref):
    n = pl.program_id(0)
    lanes = q_ref.shape[1]
    means = mean_matrix(lanes, size)
    q, k = q_ref[...], k_ref[...]
    gr = (rate_ref[...] * g_ref[...])
    w = w_ref[...]
    wz_hi, wz_lo = split(wz_ref[...])
    s_hi, s_lo = split(s_ref[0])
    o = dot(q, wz_hi) + dot(q, wz_lo) + bz_ref[...]
    o += jnp.where(seg_ref[...] == seg_before_ref[n], dot(q, s_hi) + dot(q, s_lo) + b_ref[0, 0:1, :], 0.0)
    g_hi, g_lo = split(gr)
    for mine in head_masks(q.shape, size):
        a = w * (dot_nt(only(mine, q), k) + 1.0)
        a_hi, a_lo = split(a)
        gh, gl = only(mine, g_hi), only(mine, g_lo)
        o -= dot(a_hi, gh) + dot(a_lo, gh) + dot(a_hi, gl)
    fin, inverse = layer_norm_parts(o, means)
    mixed_ref[...] = (q.astype(F32) + gain_ref[...] * fin + shift_ref[...]).astype(BF)
    fin_ref[...] = fin
    inv_ref[...] = inverse


def rows_spec(lanes):
    return pl.BlockSpec((BLK, lanes), lambda n: (n, 0))


def state_spec(*shape):
    return pl.BlockSpec((1,) + shape, lambda n: (n, 0, 0))


def whole(*shape):
    return pl.BlockSpec(shape, lambda n: (0,) * len(shape))


def out_fwd(seg_before, q, k, g, rate, seg, w, states, biases, wz, bz, gain, shift, size):
    tokens, lanes = q.shape
    rows = rows_spec(lanes)
    return pl.pallas_call(
        functools.partial(out_fwd_kernel, size),
        grid=(tokens // BLK,),
        out_shape=(
            jax.ShapeDtypeStruct((tokens, lanes), BF),
            jax.ShapeDtypeStruct((tokens, lanes), F32),
            jax.ShapeDtypeStruct((tokens, lanes), F32),
        ),
        in_specs=[smem(), rows, rows, rows, rows, rows, rows_spec(BLK), state_spec(lanes, lanes), state_spec(8, lanes),
                  whole(lanes, lanes), whole(1, lanes), whole(1, lanes), whole(1, lanes)],
        out_specs=(rows,) * 3,
        name="out_fwd",
    )(seg_before, q, k, g, rate, seg, w, states, biases, wz, bz, gain, shift)


def out_bwd_kernel(size, seg_before_ref, dmix_ref, q_ref, k_ref, v_ref, z_ref, g_ref, rate_ref, seg_ref, w_ref, s_ref, fin_ref, inv_ref, wz_ref, gain_ref, shift_ref,
                   dq_ref, do_ref, dgo_ref, alpha_ref, p_ref, p2_ref, n_ref, n2_ref, sn_ref, dgain_ref, dshift_ref):
    step = pl.program_id(0)
    lanes = q_ref.shape[1]
    means = mean_matrix(lanes, size)
    gain, shift = gain_ref[...], shift_ref[...]
    gain2 = gain * gain
    q, k = q_ref[...], k_ref[...]
    dmix = dmix_ref[...].astype(F32)
    fin = fin_ref[...]
    dfin = dmix * gain
    do = inv_ref[...] * (dfin - head_mean(dfin, means) - fin * head_mean(dfin * fin, means))
    do_ref[...] = do

    @pl.when(step == 0)
    def _():
        dgain_ref[...] = jnp.zeros_like(dgain_ref)
        dshift_ref[...] = jnp.zeros_like(dshift_ref)

    dgain_ref[...] += jnp.sum(dmix * fin, axis=0, keepdims=True)
    dshift_ref[...] += jnp.sum(dmix, axis=0, keepdims=True)
    gr = (rate_ref[...] * g_ref[...])
    w = w_ref[...]
    at = [lax.broadcasted_iota(jnp.int32, w.shape, d) // MB for d in range(2)]
    w_in = jnp.where(at[0] == at[1], w, 0.0)
    do_b = do.astype(BF)
    dq = dmix + dot_nt(do_b, wz_ref[...].astype(BF)) + jnp.where(seg_ref[...] == seg_before_ref[step], dot_nt(do_b, s_ref[0].astype(BF)), 0.0)
    gr_b = gr.astype(BF)
    dgo = jnp.zeros_like(do)
    do_hi, do_lo = split(do)
    for mine in head_masks(q.shape, size):
        da = w * dot_nt(only(mine, do_b), gr_b)
        dq -= dot(da.astype(BF), only(mine, k))
        a = w_in * (dot_nt(only(mine, q), k) + 1.0)
        a_hi, a_lo = split(a)
        dh, dl = only(mine, do_hi), only(mine, do_lo)
        dgo -= dot_tn(a_hi, dh) + dot_tn(a_lo, dh) + dot_tn(a_hi, dl)
    dq_ref[...] = dq.astype(BF)
    dgo_ref[...] = dgo
    z = z_ref[...]
    s = lax.rsqrt(head_mean(z * z, means) + EPS)
    n = z * s
    d = shift - (v_ref[...].astype(F32) - k.astype(F32))
    gs = gain * (gain * n + d)
    m2 = head_mean(gs * n, means)
    p = gs + gain2 * n
    k1, k2 = head_mean(p, means), head_mean(p * n, means) + 2.0 * m2
    ss = s * s
    alpha_ref[...] = ss * (gain2 - m2)
    p_ref[...] = p
    p2_ref[...] = ss * (p - k1 - k2 * n)
    n_ref[...] = n
    n2_ref[...] = ss * n
    sn_ref[...] = s


def out_bwd(seg_before, dmix, q, k, v, z, g, rate, seg, w, states, fin, inv, wz, gain, shift, size):
    tokens, lanes = q.shape
    rows = rows_spec(lanes)
    full = jax.ShapeDtypeStruct((tokens, lanes), F32)
    row = jax.ShapeDtypeStruct((1, lanes), F32)
    return pl.pallas_call(
        functools.partial(out_bwd_kernel, size),
        grid=(tokens // BLK,),
        out_shape=(jax.ShapeDtypeStruct((tokens, lanes), BF),) + (full,) * 8 + (row,) * 2,
        in_specs=[smem()] + [rows] * 8 + [rows_spec(BLK), state_spec(lanes, lanes), rows, rows,
                                          whole(lanes, lanes), whole(1, lanes), whole(1, lanes)],
        out_specs=(rows,) * 9 + (whole(1, lanes),) * 2,
        name="out_bwd",
    )(seg_before, dmix, q, k, v, z, g, rate, seg, w, states, fin, inv, wz, gain, shift)


def scan_bwd_kernel(size, mean_of, steps_ref, table_ref, last_ref, q_ref, k_ref, seg_ref, rate_ref, gain_ref, do_ref, dgo_ref, alpha_ref, p_ref, p2_ref, n_ref, n2_ref, sn_ref,
                    dz_ref, dg_ref, d_ref, db_ref, dzb_ref, dgb_ref, sw_ref, s2_ref, bw_ref):
    tokens, lanes = k_ref.shape
    mask = head_blocks(lanes, size)
    gain2 = gain_ref[...] * gain_ref[...]
    sw_ref[...] = jnp.zeros_like(sw_ref)
    s2_ref[...] = jnp.zeros_like(s2_ref)
    bw_ref[...] = jnp.zeros_like(bw_ref)

    def step(t, carry):
        for lane in range(2):
            m, write, slot = table_ref[lane, 0, t], table_ref[lane, 1, t], table_ref[lane, 2, t]
            rows = pl.ds(pl.multiple_of(m * MB, MB), MB)
            to = pl.ds(pl.multiple_of(write * MB, MB), MB)
            last_before, last_here = last_ref[m], last_ref[m + 1]
            q, k = q_ref[rows, :], k_ref[rows, :]
            seg = seg_ref[rows, :]
            state = sw_ref[lane]
            d_ref[slot] = state
            db_ref[slot] = bw_ref[lane]
            y = dot(jnp.concatenate([k, k], axis=1), s2_ref[lane]) + bw_ref[lane, 0:1, :]
            dg = dgo_ref[rows, :] - jnp.where(seg == last_here, y, 0.0) * (1.0 / MB)
            u = rate_ref[rows, :] * dg
            p, n = p_ref[rows, :], n_ref[rows, :]
            r1, r2, rp = mean_of(u * n), mean_of(u * gain2), mean_of(u * p)
            dz = alpha_ref[rows, :] * u - p2_ref[rows, :] * r1 - n2_ref[rows, :] * rp - sn_ref[rows, :] * (sn_ref[rows, :] * r2)
            dzb_ref[to, :] = dz
            dgb_ref[to, :] = dg
            goes = seg == last_before
            dz_c, do_c = jnp.where(goes, dz, 0.0), jnp.where(goes, do_ref[rows, :], 0.0)
            z_hi, z_lo = split(dz_c)
            o_hi, o_lo = split(do_c)
            delta = dot_tn(jnp.concatenate([k, k], axis=0), jnp.concatenate([z_hi, z_lo], axis=0))
            delta += dot_tn(jnp.concatenate([q, q], axis=0), jnp.concatenate([o_hi, o_lo], axis=0))
            keep = jnp.where(last_before == last_here, 1.0, 0.0)
            state = keep * state + jnp.where(mask, delta, 0.0)
            sw_ref[lane] = state
            s_hi, s_lo = split(state)
            s2_ref[lane] = jnp.concatenate([s_hi, s_lo], axis=0)
            bw_ref[lane] = keep * bw_ref[lane] + jnp.sum(dz_c + do_c, axis=0, keepdims=True)
        return carry

    lax.fori_loop(0, steps_ref[0], step, 0)
    dz_ref[...] = dzb_ref[0:tokens, :]
    dg_ref[...] = dgb_ref[0:tokens, :]


def scan_bwd(schedule, q, k, seg, rate, gain, parts, size, mean_of):
    steps, _, table, last = schedule
    tokens, lanes = k.shape
    blocks = tokens // BLK
    return pl.pallas_call(
        functools.partial(scan_bwd_kernel, size, mean_of),
        out_shape=(
            jax.ShapeDtypeStruct((tokens, lanes), F32),
            jax.ShapeDtypeStruct((tokens, lanes), F32),
            jax.ShapeDtypeStruct((blocks + 1, lanes, lanes), F32),
            jax.ShapeDtypeStruct((blocks + 1, 8, lanes), F32),
        ),
        in_specs=[smem()] * 3 + [vmem()] * 13,
        out_specs=(vmem(),) * 4,
        scratch_shapes=[
            pltpu.VMEM((tokens + MB, lanes), F32),
            pltpu.VMEM((tokens + MB, lanes), F32),
            pltpu.VMEM((2, lanes, lanes), F32),
            pltpu.VMEM((2, 2 * lanes, lanes), BF),
            pltpu.VMEM((2, 8, lanes), F32),
        ],
        compiler_params=pltpu.CompilerParams(vmem_limit_bytes=60 * 1024 * 1024),
        name="scan_bwd",
    )(steps, table, last, q, k, seg, rate, gain, *parts)


def post_bwd_kernel(size, seg_before_ref, q_ref, k_ref, v_ref, g_ref, rate_ref, seg_ref, w_ref, s_ref, d_ref, n_ref, sn_ref, do_ref, dz_ref, dg_ref, wz_ref, gain_ref, shift_ref,
                    dk_ref, dv_ref, dl_ref, dwz_ref, dbz_ref, dgain_ref, dshift_ref, drb_ref):
    step = pl.program_id(0)
    lanes = q_ref.shape[1]
    means = mean_matrix(lanes, size)
    gain, shift = gain_ref[...], shift_ref[...]
    q, k = q_ref[...], k_ref[...]
    rate, g, n, s = rate_ref[...], g_ref[...], n_ref[...], sn_ref[...]
    do, dz, dg = do_ref[...], dz_ref[...], dg_ref[...]
    seg = seg_ref[...]

    @pl.when(step == 0)
    def _():
        for ref in (dwz_ref, dbz_ref, dgain_ref, dshift_ref, drb_ref):
            ref[...] = jnp.zeros_like(ref)

    u = rate * dg
    dgs = s * (u - n * head_mean(u * n, means))
    de = gain * dgs
    e = gain * n + shift - (v_ref[...].astype(F32) - k.astype(F32))
    dv_ref[...] = (-de).astype(BF)
    gr = (rate * g).astype(BF)
    w = w_ref[...]
    at = [lax.broadcasted_iota(jnp.int32, w.shape, d) // MB for d in range(2)]
    w_out = jnp.where(at[0] > at[1], w, 0.0)
    do_b, dz_b = do.astype(BF), dz.astype(BF)
    dk = de + dot_nt(dz_b, wz_ref[...].astype(BF)) + jnp.where(seg == seg_before_ref[step], dot_nt(dz_b, s_ref[0].astype(BF)), 0.0)
    dk -= jnp.where(seg == seg_before_ref[step + 1], dot_nt(gr, d_ref[0].astype(BF)), 0.0) * (1.0 / MB)
    for mine in head_masks(q.shape, size):
        do_g = (w * dot_nt(only(mine, do_b), gr)).astype(BF)
        dz_g = (w_out * dot_nt(only(mine, dz_b), gr)).astype(BF)
        kh = only(mine, k)
        dk -= dot(dz_g, kh) + dot_tn(dz_g, kh) + dot_tn(do_g, only(mine, q))
    dk_ref[...] = dk.astype(BF)
    drate = head_mean(g * dg, means) * size
    dl = drate * rate * (1.0 - size * rate)
    dl_ref[...] = dl
    drb_ref[...] += jnp.sum(dl, axis=0, keepdims=True)
    dz_lo = (dz - dz_b.astype(F32)).astype(BF)
    do_lo = (do - do_b.astype(F32)).astype(BF)
    dwz_ref[...] += dot_tn(q, do_b) + dot_tn(k, dz_b) + dot_tn(q, do_lo) + dot_tn(k, dz_lo)
    dbz_ref[...] += jnp.sum(do + dz, axis=0, keepdims=True)
    dgain_ref[...] += jnp.sum(dgs * e + de * n, axis=0, keepdims=True)
    dshift_ref[...] += jnp.sum(de, axis=0, keepdims=True)


def post_bwd(seg_before, q, k, v, g, rate, seg, w, states, d_states, n, sn, do, dz, dg, wz, gain, shift, size):
    tokens, lanes = q.shape
    rows = rows_spec(lanes)
    row = jax.ShapeDtypeStruct((1, lanes), F32)
    half = jax.ShapeDtypeStruct((tokens, lanes), BF)
    return pl.pallas_call(
        functools.partial(post_bwd_kernel, size),
        grid=(tokens // BLK,),
        out_shape=(half, half, jax.ShapeDtypeStruct((tokens, lanes), F32), jax.ShapeDtypeStruct((lanes, lanes), F32), row, row, row, row),
        in_specs=[smem()] + [rows] * 6 + [rows_spec(BLK)] + [state_spec(lanes, lanes)] * 2 + [rows] * 5
        + [whole(lanes, lanes), whole(1, lanes), whole(1, lanes)],
        out_specs=(rows,) * 3 + (whole(lanes, lanes),) + (whole(1, lanes),) * 4,
        name="post_bwd",
    )(seg_before, q, k, v, g, rate, seg, w, states, d_states, n, sn, do, dz, dg, wz, gain, shift)


def prepare(segments, logits, state_init, offset_init, inner_gain, inner_shift, rate_bias):
    heads, size = offset_init.shape
    lanes = heads * size
    centred = state_init - jnp.mean(state_init, axis=-1, keepdims=True)
    wz = jnp.zeros((lanes, lanes), F32)
    for h in range(heads):
        wz = wz.at[h * size:(h + 1) * size, h * size:(h + 1) * size].set(centred[h])
    bz = (offset_init - jnp.mean(offset_init, axis=-1, keepdims=True)).reshape(1, lanes)
    rate = jnp.repeat(jax.nn.sigmoid(logits.astype(F32) + rate_bias[None, :]) / size, size, axis=1)
    seg = jnp.broadcast_to(segments[:, None], (segments.shape[0], lanes))
    seg_before = jnp.concatenate([jnp.full((1,), -1, jnp.int32), segments[BLK - 1::BLK]])
    return dict(wz=wz, bz=bz, rate=rate, seg=seg, seg_before=seg_before, w=weights_of(segments), schedule=lane_schedule(segments),
                gain=inner_gain.reshape(1, lanes), shift=inner_shift.reshape(1, lanes), size=size)


def mixer_fwd(c, q, k, v):
    mean_of = functools.partial(lane_mean, size=c["size"])
    z, g, states, biases = scan_fwd(c["schedule"], k, v, c["seg"], c["rate"], c["wz"], c["bz"], c["gain"], c["shift"], c["size"], mean_of)
    mixed, fin, inv = out_fwd(c["seg_before"], q, k, g, c["rate"], c["seg"], c["w"], states, biases, c["wz"], c["bz"], c["gain"], c["shift"], c["size"])
    return mixed, (q, k, v, z, g, states, fin, inv)


def mixer_bwd(c, kept, dmix):
    mean_of = functools.partial(lane_mean, size=c["size"])
    q, k, v, z, g, states, fin, inv = kept
    size = c["size"]
    dq, do, dgo, alpha, p, p2, n, n2, sn, dgain, dshift = out_bwd(
        c["seg_before"], dmix, q, k, v, z, g, c["rate"], c["seg"], c["w"], states, fin, inv, c["wz"], c["gain"], c["shift"], size)
    dz, dg, d_states, _ = scan_bwd(c["schedule"], q, k, c["seg"], c["rate"], c["gain"], (do, dgo, alpha, p, p2, n, n2, sn), size, mean_of)
    dk, dv, dl, dwz, dbz, dgain2, dshift2, drb = post_bwd(
        c["seg_before"], q, k, v, g, c["rate"], c["seg"], c["w"], states, d_states, n, sn, do, dz, dg, c["wz"], c["gain"], c["shift"], size)
    heads = q.shape[1] // size
    dstate = jnp.stack([dwz[h * size:(h + 1) * size, h * size:(h + 1) * size] for h in range(heads)])
    by_head = lambda row: row.reshape(heads, size)
    return (dq, dk, dv, dl[:, ::size].astype(BF), dstate, by_head(dbz), by_head(dgain + dgain2), by_head(dshift + dshift2), drb.reshape(heads, size)[:, 0])


def rms_piece(values, gain):
    return values * lax.rsqrt(jnp.mean(values * values, axis=-1, keepdims=True) + EPS) * gain


def gelu_piece(values):
    return jax.nn.gelu(values, approximate=True)


def product(left, right):
    return jnp.dot(left, right, preferred_element_type=F32)


def outer_sum(left, right):
    return lax.dot_general(left, right, (((0,), (0,)), ((), ())), preferred_element_type=F32)


def back_product(left, right):
    return lax.dot_general(left, right, (((1,), (1,)), ((), ())), preferred_element_type=F32)


def swap(values, axis, mask):
    return lax.ppermute(values, axis, [(i, i ^ mask) for i in range(lax.axis_size(axis))])


def halving_orders():
    rows = [("row", 1 << i) for i in range(lax.axis_size("row").bit_length() - 1)]
    seqs = [("seq", 1 << i) for i in range(lax.axis_size("seq").bit_length() - 1)]
    core, xs = rows[:1], rows[1:]
    cut = len(seqs) // 2
    ys, zs = seqs[:cut], seqs[cut:]
    return (core + xs + ys + zs, core + ys + zs[:1] + xs + zs[1:], core + zs[:1] + xs + ys + zs[1:])


def relative_order(order, features):
    blocks = 1 << len(order)
    at = np.arange(features) // (features // blocks)
    flips = {"row": np.zeros(features, np.int32), "seq": np.zeros(features, np.int32)}
    for i, (axis, mask) in enumerate(order):
        flips[axis] += ((at >> (len(order) - 1 - i)) & 1) * mask
    block = (lax.axis_index("row") ^ flips["row"]) * lax.axis_size("seq") + (lax.axis_index("seq") ^ flips["seq"])
    source = block * (features // blocks) + np.arange(features) % (features // blocks)
    return (jnp.arange(features)[:, None] == source[None, :]).astype(BF)


def reduce_outer(left, right, order):
    half = left.shape[1] // 2
    send = outer_sum(left[:, half:], right).astype(BF)
    keep = outer_sum(left[:, :half], right).astype(BF)
    for axis, mask in order[:-1]:
        got = swap(send, axis, mask)
        half = half // 2
        send = (keep[half:].astype(F32) + got[half:].astype(F32)).astype(BF)
        keep = (keep[:half].astype(F32) + got[:half].astype(F32)).astype(BF)
    axis, mask = order[-1]
    return keep.astype(F32) + swap(send, axis, mask).astype(F32)


def shards(
    tokens_in, segment_ids, norm_in_gain, query_weight, key_weight, value_weight, rate_weight, gate_weight, out_weight,
    state_init, offset_init, inner_gain, inner_shift, rate_bias, norm_post_gain, norm_mlp_gain, ffn_gate, ffn_up, ffn_down, cotangent,
):
    row_count, token_count, features = tokens_in.shape
    assert row_count == 1
    groups = lax.axis_size("seq")
    heads_here, size = offset_init.shape
    lanes = heads_here * size
    flat_in = tokens_in[0].astype(F32)
    normed_f, norm_in_pull = jax.vjp(rms_piece, flat_in, norm_in_gain)
    normed_in = normed_f.astype(BF)

    def to_heads(values):
        width = values.shape[1] // groups
        split_up = jnp.swapaxes(values.astype(BF).reshape(token_count, groups, width), 0, 1)
        return lax.all_to_all(split_up, "seq", split_axis=0, concat_axis=0, tiled=True).reshape(groups * token_count, width)

    def to_tokens(values):
        width = values.shape[1]
        moved = lax.all_to_all(values.reshape(groups, token_count, width), "seq", split_axis=0, concat_axis=0, tiled=True)
        return jnp.swapaxes(moved, 0, 1).reshape(token_count, groups * width)

    k_heads = to_heads(product(normed_in, key_weight))
    v_heads = to_heads(product(normed_in, value_weight))
    r_heads = to_heads(product(normed_in, rate_weight))
    q_heads = to_heads(product(normed_in, query_weight))
    parts = prepare(segment_ids[0], r_heads, state_init, offset_init, inner_gain, inner_shift, rate_bias)
    mixed_heads, kept = mixer_fwd(parts, q_heads, k_heads, v_heads)
    mixed_f = to_tokens(mixed_heads).astype(F32)
    post_norm, post_pull = jax.vjp(rms_piece, mixed_f, norm_post_gain)
    gate_pre = product(normed_in, gate_weight)
    gelu_out, gelu_pull = jax.vjp(gelu_piece, gate_pre)
    branch = (post_norm * gelu_out).astype(BF)
    middle = flat_in + product(branch, out_weight)
    normed_mid_f, mid_pull = jax.vjp(rms_piece, middle, norm_mlp_gain)
    normed_mid = normed_mid_f.astype(BF)
    gate_proj = product(normed_mid, ffn_gate)
    up_proj = product(normed_mid, ffn_up)
    silu_out, silu_pull = jax.vjp(jax.nn.silu, gate_proj)
    hidden = (silu_out * up_proj).astype(BF)
    block_out = (middle + product(hidden, ffn_down)).astype(BF)
    grad_ffn = cotangent[0]
    grad_out = grad_ffn.astype(F32)
    order_a, order_b, order_c = halving_orders()
    rel_a, rel_b, rel_c = [relative_order(order, features) for order in (order_a, order_b, order_c)]

    def put(values, rel):
        return product(values, rel).astype(BF)

    grad_down = reduce_outer(put(grad_ffn, rel_a), hidden, order_a).T
    grad_hidden = back_product(grad_ffn, ffn_down)
    grad_gate_proj = silu_pull(grad_hidden * up_proj)[0].astype(BF)
    grad_up_proj = (grad_hidden * silu_out).astype(BF)
    grad_ffn_gate = reduce_outer(put(normed_mid, rel_b), grad_gate_proj, order_b)
    grad_ffn_up = reduce_outer(put(normed_mid, rel_c), grad_up_proj, order_c)
    grad_normed_mid = back_product(grad_gate_proj, ffn_gate) + back_product(grad_up_proj, ffn_up)
    grad_mid_part, grad_norm_mlp = mid_pull(grad_normed_mid)
    grad_middle = grad_out + grad_mid_part
    grad_branch_out = grad_middle.astype(BF)
    grad_out_proj = reduce_outer(put(branch, rel_a), grad_branch_out, order_a)
    grad_branch = back_product(grad_branch_out, out_weight)
    grad_gate_pre = gelu_pull(grad_branch * post_norm)[0].astype(BF)
    in_a, in_b, in_c = put(normed_in, rel_a), put(normed_in, rel_b), put(normed_in, rel_c)
    grad_gate = reduce_outer(in_b, grad_gate_pre, order_b)
    grad_mixed_part, grad_norm_post = post_pull(grad_branch * gelu_out)
    grad_heads = to_heads(grad_mixed_part)
    grad_q, grad_k, grad_v, grad_r, grad_state, grad_offset, grad_igain, grad_ishift, grad_rbias = mixer_bwd(parts, kept, grad_heads)
    grad_q_flat = to_tokens(grad_q)
    grad_query = reduce_outer(in_c, grad_q_flat, order_c)
    grad_k_flat = to_tokens(grad_k)
    grad_v_flat = to_tokens(grad_v)
    grad_r_flat = to_tokens(grad_r)
    grad_key = reduce_outer(in_a, grad_k_flat, order_a)
    grad_value_rate = reduce_outer(in_b, jnp.concatenate([grad_v_flat, grad_r_flat], axis=1), order_b)
    grad_value, grad_rate = grad_value_rate[:, :features], grad_value_rate[:, features:]
    by_head = jnp.concatenate(
        [grad_state.reshape(heads_here, -1), grad_offset, grad_igain, grad_ishift, jnp.broadcast_to(grad_rbias[:, None], (heads_here, size))], axis=1
    ).reshape(-1, lanes)
    mask = 1
    while mask < lax.axis_size("row"):
        by_head = by_head + swap(by_head, "row", mask)
        mask *= 2
    by_head = by_head.reshape(heads_here, -1)
    cuts = [size * size + i * size for i in range(4)]
    grad_normed_in = (
        back_product(grad_q_flat, query_weight)
        + back_product(grad_k_flat, key_weight)
        + back_product(grad_v_flat, value_weight)
        + back_product(grad_r_flat, rate_weight)
        + back_product(grad_gate_pre, gate_weight)
    )
    grad_in_part, grad_norm_in = norm_in_pull(grad_normed_in)
    grad_tokens = grad_middle + grad_in_part
    devices = groups * lax.axis_size("row")
    gains = jnp.stack([grad_norm_in, grad_norm_post, grad_norm_mlp]).reshape(3, devices, features // devices)
    gains = jnp.swapaxes(gains, 0, 1).reshape(devices, -1)
    gains = jnp.sum(lax.all_to_all(gains, ("row", "seq"), split_axis=0, concat_axis=0, tiled=True), axis=0).reshape(3, -1)
    return (
        block_out[None], grad_tokens[None], gains[0], grad_query, grad_key, grad_value, grad_rate, grad_gate, grad_out_proj,
        by_head[:, :cuts[0]].reshape(heads_here, size, size), by_head[:, cuts[0]:cuts[1]], by_head[:, cuts[1]:cuts[2]],
        by_head[:, cuts[2]:cuts[3]], by_head[:, cuts[3]], gains[1], gains[2], grad_ffn_gate, grad_ffn_up, grad_down,
    )


def solution(mesh):
    whole_copy, tokens, heads = P(), P("row", "seq", None), P("seq")
    both = P(("row", "seq"))
    return jax.shard_map(
        shards,
        mesh=mesh,
        in_specs=(tokens, P("row", None)) + (whole_copy,) * 7 + (heads,) * 5 + (whole_copy,) * 5 + (tokens,),
        out_specs=(tokens, tokens) + (both,) * 7 + (heads,) * 5 + (both,) * 4 + (P(None, ("row", "seq")),),
        check_vma=False,
    )
```
